32 devices in a mesh: dp: 4 (over x, core), section: 2 (over y), expert: 4 (over z).
Axes of the slice: x: 2, y: 2, z: 4, core: 2. Of those that a mesh axis runs over, the one named last changes fastest.
Arguments:
- paths_in: bfloat16 [2, 256, 4, 7168], P(None, 'expert', None, 'dp'), may hold values from -12 to 12
- path_proj: bfloat16 [2, 24, 4, 7168], P('section', None, None, 'dp'), may hold values from -0.03125 to 0.03125
- coef_bias: float32 [2, 24], P('section'), may hold values from -4 to 4
- norm_gain: bfloat16 [2, 7168], P('section', 'dp'), may hold values from 0.25 to 1.75
- w_gate_up: bfloat16 [2, 4, 7168, 2, 512], P('section', 'expert', 'dp'), may hold values from -0.0625 to 0.0625
- w_down: bfloat16 [2, 4, 512, 7168], P('section', 'expert', None, 'dp'), may hold values from -0.1875 to 0.1875
- routes: int32 [2, 2, 256, 1], P('section', None, 'expert'), may hold values from 0 to 1; in each aligned block of 64 rows (0 to 63, 64 to 127, ..., all dimensions but the last counted through in order) at most 32 rows name the same one
- route_gate: float32 [2, 2, 256, 1], P('section', None, 'expert'), may hold values from 0.2 to 1
Outputs:
- paths_out: bfloat16 [2, 2, 256, 4, 7168], P('section', None, 'expert', None, 'dp')
The draws below stay inside these ranges and needn't reach their ends.
Inputs may be any that keep to these rules, and one draw needn't show every extreme that they name: `routes`: each row names exactly one expert. In each aligned block of 64 rows (the tokens of one index of expert in one layer and micro-batch) no expert is named more than 32 times, a bound that some block reaches.
All inputs are finite; a program needn't handle non-finite values.
Results may differ from the reference program's by a relative error of at most 0.014.
Values may be sent and summed in bfloat16 or wider, within the bound.
A program may use at most 64 MiB of HBM per device.

```python
import math
import jax
import jax.numpy as jnp
import numpy as np
from jax import lax

D = 7168
RESIDUAL_STREAMS = 4
FFE = 1024
SINK = 20
MB = 2
TOPK = 1
ROWS = 64
LAYERS = 2
EXPERTS = 2
TOKENS = 256
CAP = 32
NCOEF = 24
N_EXPERT = 4


def draw_paths_in(key, part):
    shape = (MB, TOKENS, RESIDUAL_STREAMS, D)
    position = jnp.arange(D, dtype=jnp.float32) / D - 0.5
    rough_key = jax.random.fold_in(key, 11)
    value_key = jax.random.fold_in(key, 12)
    rough = jnp.exp(jax.random.uniform(rough_key, (D,), jnp.float32, -0.35, 0.35))
    column_scale = jnp.exp(jnp.log(3.0) * position) * rough
    values = jnp.clip(jax.random.normal(value_key, shape, jnp.float32), -4.0, 4.0)
    return (values * column_scale).astype(jnp.bfloat16)


def block_levels(rng, extent, shards, least, high):
    def one(axis_at, shards_of):
        draws = jax.random.uniform(jax.random.fold_in(jax.random.fold_in(rng, 6), axis_at), (shards_of,), jnp.float32, least / len(shards), high / len(shards))
        return jnp.repeat(jnp.exp(draws), extent[axis_at] // shards_of).reshape((-1,) + (1,) * (len(extent) - axis_at - 1))

    loudness = one(*shards[0])
    for cut in shards[1:]:
        loudness = loudness * one(*cut)
    return loudness


def assign_block(own_key, own, number, rows, amount, top, reach, slope):
    ranking = jax.random.permutation(own_key, amount)
    packed, usual = portions_of(amount, rows * top, reach, slope, True), portions_of(amount, rows * top, reach, slope, False)
    places = jnp.arange(amount)

    def named(lengths, rotation):
        used = int((lengths > 0).sum())
        fixed = max(1, used // 4)
        passed = fixed + (places - fixed + rotation * (used - fixed)) % max(1, amount - fixed)
        return jnp.zeros((amount,), jnp.int32).at[ranking[jnp.where(places < fixed, places, passed)]].set(jnp.asarray(lengths, jnp.int32))

    lengths = jnp.where(number % 4 == 0, named(packed, number // 4), named(usual, number - number // 4 - 1))
    mixed = jax.random.permutation(jax.random.fold_in(own, 3), amount)
    donor, sink = mixed[0:amount // 2 * 2:2], mixed[1:amount // 2 * 2:2]
    slack = jnp.minimum(lengths[donor] - 1, reach - lengths[sink]) // 2
    slack = jnp.where((donor == ranking[0]) | (sink == ranking[0]) | (lengths[sink] == 0), 0, jnp.maximum(slack, 0))
    passed = jax.random.randint(jax.random.fold_in(own, 4), (amount // 2,), 0, 1 << 20) % (slack + 1)
    lengths = lengths.at[donor].add(-passed).at[sink].add(passed)
    items = jnp.searchsorted(jnp.cumsum(lengths), jnp.arange(rows * top), side="right").astype(jnp.int32)
    grid = items.reshape(top, rows).T
    grid = grid[jax.random.permutation(jax.random.fold_in(own, 1), rows)]
    rotation = jax.random.randint(jax.random.fold_in(own, 2), (rows, 1), 0, top)
    return jnp.take_along_axis(grid, (jnp.arange(top)[None, :] + rotation) % top, axis=1)


def portions_of(amount, total, limit, skew, full):
    weights = [(1 << 20) // math.isqrt(grade ** skew) + 1 for grade in range(1, amount + 1)]
    largest = limit if full else min(limit, max(-(-total // amount), total * weights[0] // sum(weights)))
    least = 1 if total - largest >= amount - 1 else 0
    counts, rest = [largest] + [least] * (amount - 1), total - largest - least * (amount - 1)
    while rest > 0:
        movable = [i for i in range(1, amount) if counts[i] < largest] or [i for i in range(1, amount) if counts[i] < limit]
        whole, left = sum([weights[i] for i in movable]), rest
        for i in movable:
            addition = min(limit - counts[i], max(1, left * weights[i] // whole), rest)
            counts[i] = counts[i] + addition
            rest = rest - addition
    return np.array(counts)


def bell_draw(rng, dims, scale, reach, shards=(), held_as=jnp.bfloat16):
    entries = scale * jax.random.normal(rng, dims, jnp.float32)
    if shards:
        entries = entries * block_levels(rng, dims, shards, -0.22, 0.18)
    return jnp.clip(entries, -reach, reach).astype(held_as)


def setup_inputs(seed: int = 0) -> dict:
    key_of = jax.random.split(jax.random.key(seed), 9)
    paths_in = draw_paths_in(jax.random.fold_in(key_of[8], 71), 0)
    path_proj = bell_draw(key_of[1], (LAYERS, NCOEF, RESIDUAL_STREAMS, D), (RESIDUAL_STREAMS * D) ** -0.5, 0.03125, ((0, 2), (3, 4)))
    coef_bias = bell_draw(key_of[2], (LAYERS, NCOEF), 1.0, 4.0, ((0, 2),), jnp.float32)
    norm_gain = jnp.clip(1.0 + 0.15 * jax.random.normal(key_of[3], (LAYERS, D), jnp.float32), 0.25, 1.75).astype(jnp.bfloat16)
    w_gate_up = bell_draw(key_of[4], (LAYERS, 2 * EXPERTS, D, 2, FFE // 2), D ** -0.5, 0.0625, ((0, 2), (1, 4), (2, 4)))
    w_down = bell_draw(key_of[5], (LAYERS, 2 * EXPERTS, FFE // 2, D), FFE ** -0.5, 0.1875, ((0, 2), (1, 4), (3, 4)))
    routes_keys = jax.random.split(jax.random.fold_in(key_of[6], 1), LAYERS * MB * TOKENS // ROWS)
    routes_turns = jax.random.permutation(jax.random.fold_in(key_of[6], 3), LAYERS * MB * TOKENS // ROWS)
    routes = jax.vmap(lambda own, number: assign_block(jax.random.fold_in(key_of[6], 2), own, number, ROWS, EXPERTS, TOPK, CAP, 1))(routes_keys, routes_turns).reshape((LAYERS, MB, TOKENS, TOPK))
    route_gate = jnp.clip(0.2 + 0.8 * jax.random.uniform(key_of[7], (LAYERS, MB, TOKENS, TOPK), jnp.float32) ** block_levels(key_of[7], (LAYERS, MB, TOKENS, TOPK), ((0, 2), (2, 4)), -0.2, 0.2), 0.2, 1.0)
    return dict(paths_in=paths_in, path_proj=path_proj, coef_bias=coef_bias, norm_gain=norm_gain, w_gate_up=w_gate_up, w_down=w_down, routes=routes, route_gate=route_gate)


EPSILON = 1e-06

def doubly_stochastic_project(stream_mixer):
    for repeat in range(SINK):
        stream_mixer = stream_mixer / lax.optimization_barrier(jnp.sum(stream_mixer, axis=2, keepdims=True))
        stream_mixer = stream_mixer / lax.optimization_barrier(jnp.sum(stream_mixer, axis=1, keepdims=True))
    return stream_mixer

def expert_layer(normed, routes_now, gates_now, gate_probabilities, down_weights):
    row_bound = N_EXPERT * CAP
    half_units = FFE // 2
    gate_pairs = gate_probabilities.reshape(EXPERTS, 2, D, 2 * half_units)
    down_pairs = down_weights.reshape(EXPERTS, 2, half_units, D)

    def one_expert(running, inputs):
        gate_up, down_proj, expert_id = inputs
        chosen = routes_now == expert_id
        weight = lax.optimization_barrier(jnp.sum(jnp.where(chosen, gates_now, 0.0), axis=1))
        routed = jnp.any(chosen, axis=1)
        picked_rows = jnp.argsort(jnp.where(routed, 0, 1).astype(jnp.int32), stable=True)[:row_bound]
        picked = normed[picked_rows]
        expert_output_rows = jnp.zeros((row_bound, D), jnp.float32)
        for half in range(2):
            hidden_pre = jnp.dot(picked, gate_up[half], preferred_element_type=jnp.float32)
            hidden = (jax.nn.silu(hidden_pre[:, :half_units]) * hidden_pre[:, half_units:]).astype(jnp.bfloat16)
            half_out = jnp.dot(hidden, down_proj[half], preferred_element_type=jnp.float32).astype(jnp.bfloat16)
            expert_output_rows = expert_output_rows + lax.optimization_barrier(half_out).astype(jnp.float32)
        scaled = weight[picked_rows][:, None] * expert_output_rows
        return (running.at[picked_rows].add(scaled), None)
    start_value = jnp.zeros((normed.shape[0], D), jnp.float32)
    expert_ids = jnp.arange(EXPERTS, dtype=jnp.int32)
    running, unused = lax.scan(one_expert, start_value, (gate_pairs, down_pairs, expert_ids))
    return running

def mix_layer(residual, path_proj, coef_bias, norm_gain, gate_probabilities, down_weights, routes_now, gates_now):
    widened = residual.astype(jnp.float32)
    square_mean = lax.optimization_barrier(jnp.mean(widened * widened, axis=(1, 2)))
    projected = jnp.einsum('tsd,csd->tc', widened, path_proj.astype(jnp.float32), precision=lax.Precision.HIGHEST)
    router_scores = projected * lax.rsqrt(square_mean + EPSILON)[:, None] + coef_bias[None, :]
    pre_weight = jax.nn.sigmoid(router_scores[:, :RESIDUAL_STREAMS])
    post_weight = 2.0 * jax.nn.sigmoid(router_scores[:, RESIDUAL_STREAMS:2 * RESIDUAL_STREAMS])
    stream_mixer = doubly_stochastic_project(jnp.exp(router_scores[:, 2 * RESIDUAL_STREAMS:]).reshape(-1, RESIDUAL_STREAMS, RESIDUAL_STREAMS))
    merged = lax.optimization_barrier(jnp.sum(pre_weight[:, :, None] * widened, axis=1))
    width_mean = lax.optimization_barrier(jnp.mean(merged * merged, axis=1))
    normed = (merged * lax.rsqrt(width_mean + EPSILON)[:, None] * norm_gain.astype(jnp.float32)[None, :]).astype(jnp.bfloat16)
    branch = expert_layer(normed, routes_now, gates_now, gate_probabilities, down_weights)
    carried = jnp.einsum('tji,tid->tjd', stream_mixer, widened, precision=lax.Precision.HIGHEST)
    return (carried + post_weight[:, :, None] * branch[:, None, :]).astype(jnp.bfloat16)

def reference(paths_in, path_proj, coef_bias, norm_gain, w_gate_up, w_down, routes, route_gate):
    per_micro = []
    for micro_index in range(MB):
        residual = paths_in[micro_index]
        layer_outputs = []
        for layer_index in range(LAYERS):
            residual = mix_layer(residual, path_proj[layer_index], coef_bias[layer_index], norm_gain[layer_index], w_gate_up[layer_index], w_down[layer_index], routes[layer_index, micro_index], route_gate[layer_index, micro_index])
            layer_outputs.append(residual)
        per_micro.append(jnp.stack(layer_outputs))
    return jnp.stack(per_micro, axis=1)
```

```python
import functools

import jax
import jax.numpy as jnp
from jax import lax
from jax.experimental import pallas as pl
from jax.experimental.pallas import tpu as pltpu
from jax.sharding import PartitionSpec as P

SINK = 20
EPSILON = 1e-06
MESH = pl.DeviceIdType.MESH
F32 = jnp.float32
BF16 = jnp.bfloat16
LANES = 128
NT = (((1,), (1,)), ((), ()))


def kernel(
    sizes,
    paths_ref, proj_ref, bias_ref, gain_ref, gate_up_ref, down_ref, routes_ref, gates_ref,
    out_ref,
    path, wgu, wd, stats, crow, tab, slotcol, outgoing, recv, acc, part, rs_recv, hid, half_out, ret,
    branch, acc_branch, in_crow, in_branch, obuf,
    load_sem, out_sem, st_s, st_r, di_s, di_r, rs_s, rs_r, ag_s, ag_r, re_s, re_r, se_s, se_r,
):
    micro, streams, rows, width, coefs, inner, cap, n_dp, n_ex, n_sec, depth = sizes
    experts = n_ex // 2
    slots = experts * cap
    items = n_ex * cap
    share = items // n_dp
    shift = cap.bit_length() - 1
    dp, ex, sec = (lax.axis_index(a) for a in ("dp", "expert", "section"))
    pre0, post0, scale0, mix0 = 0, streams, 2 * streams, 2 * streams + 1

    barrier = pltpu.get_barrier_semaphore()
    greeted = 0
    for name, me, count in (("dp", dp, n_dp), ("expert", ex, n_ex), ("section", sec, n_sec)):
        for off in range(1, count):
            pl.semaphore_signal(
                barrier, inc=1, device_id={name: lax.rem(me + off, count)}, device_id_type=MESH
            )
            greeted += 1

    loads = [
        pltpu.make_async_copy(paths_ref.at[m], path.at[m], load_sem.at[m]) for m in range(micro)
    ]
    load_gu = pltpu.make_async_copy(gate_up_ref, wgu, load_sem.at[micro])
    load_d = pltpu.make_async_copy(down_ref, wd, load_sem.at[micro + 1])
    for c in (*loads, load_gu, load_d):
        c.start()

    def remote(src, dst, send, receive, name, target):
        return pltpu.make_async_remote_copy(
            src_ref=src, dst_ref=dst, send_sem=send, recv_sem=receive,
            device_id={name: target}, device_id_type=MESH,
        )

    eye = lax.broadcasted_iota(jnp.int32, (rows, rows), 0) == lax.broadcasted_iota(
        jnp.int32, (rows, rows), 1
    )
    below = (
        lax.broadcasted_iota(jnp.int32, (rows, rows), 1)
        < lax.broadcasted_iota(jnp.int32, (rows, rows), 0)
    )

    def columns(table_ref, first, last):
        turned = jnp.transpose(table_ref[...])
        for k in range(first, last):
            tab[k] = jnp.broadcast_to(turned[:rows, k : k + 1], (rows, LANES))

    def mixed(m, c, added):
        cols = pl.ds(pl.multiple_of(c * LANES, LANES), LANES)
        p = [path[m, i, :, cols].astype(F32) for i in range(streams)]
        res = []
        for j in range(streams):
            total = tab[post0 + j] * added(cols)
            for i in range(streams):
                total = total + tab[mix0 + j * streams + i] * p[i]
            res.append(total.astype(BF16))
        return cols, res

    def stage_stats(m):
        loads[m].wait()
        for layer in range(n_sec - 1):
            @pl.when(sec > layer)
            def _():
                remote(crow.at[m], in_crow.at[m, layer], se_s.at[m, 0, 0],
                       se_r.at[m, layer, 0], "section", layer).wait_recv()
                columns(in_crow.at[m, layer], post0, mix0 + streams * streams)
                remote(branch.at[m], in_branch.at[m, layer], se_s.at[m, 0, 1],
                       se_r.at[m, layer, 1], "section", layer).wait_recv()

                @pl.loop(0, width // LANES)
                def _(c):
                    cols, res = mixed(m, c, lambda s: in_branch[m, layer, :, s].astype(F32))
                    for j in range(streams):
                        path[m, j, :, cols] = res[j]

        projected = jnp.zeros((coefs, rows), F32)
        at = coefs
        for j in range(streams):
            pj = path[m, j]
            projected = projected + lax.dot_general(
                proj_ref[j], pj, NT, preferred_element_type=F32
            )
            for i in range(j + 1):
                g = lax.dot_general(path[m, i], pj, NT, preferred_element_type=F32)
                stats[m, dp, at : at + 1, :] = jnp.sum(jnp.where(eye, g, 0.0), axis=0, keepdims=True)
                at += 1
        stats[m, dp, :coefs, :] = projected
        if m == 0:
            pl.semaphore_wait(barrier, greeted)
        return [
            remote(stats.at[m, dp], stats.at[m, dp], st_s.at[m, off - 1], st_r.at[m, off - 1],
                   "dp", lax.rem(dp + off, n_dp))
            for off in range(1, n_dp)
        ]

    def await_from(m, buf, sems, name, me, count):
        for off in range(1, count):
            source = lax.rem(me + count - off, count)
            remote(buf.at[m, source], buf.at[m, source], sems[0].at[m, off - 1],
                   sems[1].at[m, off - 1], name, source).wait_recv()

    def stage_dispatch(m):
        await_from(m, stats, (st_s, st_r), "dp", dp, n_dp)
        total = stats[m, 0]
        for d in range(1, n_dp):
            total = total + stats[m, d]
        gram, at = {}, coefs
        for j in range(streams):
            for i in range(j + 1):
                gram[i, j] = total[at : at + 1]
                at += 1
        square = gram[0, 0]
        for i in range(1, streams):
            square = square + gram[i, i]
        bias_eye = lax.broadcasted_iota(jnp.int32, (coefs, coefs), 0) == lax.broadcasted_iota(
            jnp.int32, (coefs, coefs), 1
        )
        bias = jnp.sum(jnp.where(bias_eye, bias_ref[...], 0.0), axis=1, keepdims=True)
        logits = total[:coefs] * lax.rsqrt(square * (1.0 / (streams * depth)) + EPSILON) + bias
        weights = jax.nn.sigmoid(logits[: 2 * streams])
        crow[m, pre0:streams, :rows] = weights[:streams]
        crow[m, post0 : 2 * streams, :rows] = 2.0 * weights[streams:]
        norm = jnp.zeros_like(square)
        for i, j in gram:
            pair = weights[i : i + 1] * weights[j : j + 1] * gram[i, j]
            norm = norm + (pair if i == j else 2.0 * pair)
        crow[m, scale0 : scale0 + 1, :rows] = lax.rsqrt(norm * (1.0 / depth) + EPSILON)
        columns(crow.at[m], pre0, scale0 + 1)

        route = routes_ref[m]
        lane = lax.broadcasted_iota(jnp.int32, (rows, LANES), 1)
        chosen = (lane == route).astype(F32)
        earlier = jnp.dot(
            below.astype(F32).astype(BF16), chosen.astype(BF16), preferred_element_type=F32
        )
        rank = jnp.sum(earlier * chosen, axis=1, keepdims=True)
        slot = route.astype(F32) * cap + rank
        slotcol[m] = slot
        slotrow = jnp.sum(jnp.where(eye, slot, 0.0), axis=0, keepdims=True)
        pick = (
            lax.broadcasted_iota(jnp.int32, (slots, rows), 0).astype(F32) == slotrow
        ).astype(F32).astype(BF16)

        @pl.loop(0, width // LANES)
        def _(c):
            cols = pl.ds(pl.multiple_of(c * LANES, LANES), LANES)
            merged = tab[pre0] * path[m, 0, :, cols].astype(F32)
            for i in range(1, streams):
                merged = merged + tab[pre0 + i] * path[m, i, :, cols].astype(F32)
            normed = (merged * tab[scale0] * gain_ref[:, cols].astype(F32)).astype(BF16)
            moved = jnp.dot(pick, normed, preferred_element_type=F32).astype(BF16)
            outgoing[m, :, :, cols] = moved.reshape(experts, cap, LANES)

        copies = []
        for off in range(1, n_ex):
            target = lax.rem(ex + off, n_ex)
            copies.append(
                remote(outgoing.at[m, lax.div(target, 2)], recv.at[m, ex], di_s.at[m, off - 1],
                       di_r.at[m, off - 1], "expert", target)
            )
            copies[-1].start()
        recv[m, ex] = outgoing[m, lax.div(ex, 2)]

        start = jnp.exp(logits[2 * streams :])
        entries = tuple(start[k : k + 1] for k in range(streams * streams))

        def balance(_, a):
            a = list(a)
            for groups in (
                [[j * streams + i for i in range(streams)] for j in range(streams)],
                [[j * streams + i for j in range(streams)] for i in range(streams)],
            ):
                for group in groups:
                    inverse = 1.0 / functools.reduce(jnp.add, [a[k] for k in group])
                    for k in group:
                        a[k] = a[k] * inverse
            return tuple(a)

        entries = lax.fori_loop(0, SINK, balance, entries)
        for k in range(streams * streams):
            crow[m, mix0 + k : mix0 + k + 1, :rows] = entries[k]
        to_sections(m, crow, in_crow, 0, "start")
        return copies

    def to_sections(m, src, dst, kind, act):
        for off in range(1, n_sec):
            @pl.when(sec + off < n_sec)
            def _():
                copy = remote(src.at[m], dst.at[m, sec], se_s.at[m, off - 1, kind],
                              se_r.at[m, sec, kind], "section", sec + off)
                copy.start() if act == "start" else copy.wait_send()

    def stage_up(m):
        await_from(m, recv, (di_s, di_r), "expert", ex, n_ex)
        if m == 0:
            load_gu.wait()
        tile = 256

        @pl.loop(0, 2 * inner // tile)
        def _(c):
            cols = pl.ds(pl.multiple_of(c * tile, tile), tile)
            product = jnp.dot(
                recv[m].reshape(items, width), wgu[:, cols], preferred_element_type=F32
            )
            acc[m, :, :, cols] = product.reshape(n_dp, share, tile)
            part[m, :, :, cols] = product.astype(BF16).reshape(n_dp, share, tile)

        return [
            remote(part.at[m, lax.rem(dp + off, n_dp)], rs_recv.at[m, off - 1],
                   rs_s.at[m, off - 1], rs_r.at[m, off - 1], "dp", lax.rem(dp + off, n_dp))
            for off in range(1, n_dp)
        ]

    def stage_hidden(m):
        for off in range(1, n_dp):
            remote(part.at[m, 0], rs_recv.at[m, off - 1], rs_s.at[m, off - 1],
                   rs_r.at[m, off - 1], "dp", lax.rem(dp + off, n_dp)).wait_recv()
        total = acc[m, dp]
        for off in range(1, n_dp):
            total = total + rs_recv[m, off - 1].astype(F32)
        gate = total[:, :inner]
        hid[m, dp] = (gate * jax.nn.sigmoid(gate) * total[:, inner:]).astype(BF16)
        return [
            remote(hid.at[m, dp], hid.at[m, dp], ag_s.at[m, off - 1], ag_r.at[m, off - 1],
                   "dp", lax.rem(dp + off, n_dp))
            for off in range(1, n_dp)
        ]

    def stage_down(m):
        await_from(m, hid, (ag_s, ag_r), "dp", dp, n_dp)
        if m == 0:
            load_d.wait()
        tile = 256 if width % 256 == 0 else LANES

        @pl.loop(0, width // tile)
        def _(c):
            cols = pl.ds(pl.multiple_of(c * tile, tile), tile)
            product = jnp.dot(
                hid[m].reshape(items, inner), wd[:, cols], preferred_element_type=F32
            )
            half_out[m, :, :, cols] = product.astype(BF16).reshape(n_ex, cap, tile)

        copies = [
            remote(half_out.at[m, lax.rem(ex + off, n_ex)], ret.at[m, ex], re_s.at[m, off - 1],
                   re_r.at[m, off - 1], "expert", lax.rem(ex + off, n_ex))
            for off in range(1, n_ex)
        ]
        for copy in copies:
            copy.start()
        ret[m, ex] = half_out[m, ex]
        return copies

    def stage_combine(m):
        columns(crow.at[m], post0, mix0 + streams * streams)
        place = lax.broadcasted_iota(jnp.int32, (rows, items), 1)
        place = ((place >> (shift + 1)) << shift) + (place & (cap - 1))
        back = (place.astype(F32) == slotcol[m]).astype(F32).astype(BF16)
        gates = gates_ref[m]
        await_from(m, ret, (re_s, re_r), "expert", ex, n_ex)
        tile = 256 if width % 256 == 0 else LANES

        @pl.loop(0, width // tile)
        def _(c):
            cols = pl.ds(pl.multiple_of(c * tile, tile), tile)
            value = gates * jnp.dot(
                back, ret[m, :, :, cols].reshape(items, tile), preferred_element_type=F32
            )
            acc_branch[:, cols] = value
            branch[m, :, cols] = value.astype(BF16)

        to_sections(m, branch, in_branch, 1, "start")

        @pl.loop(0, width // LANES)
        def _(c):
            cols, res = mixed(m, c, lambda s: acc_branch[:, s])
            for j in range(streams):
                obuf[m, j, :, cols] = res[j]

        pltpu.make_async_copy(obuf.at[m], out_ref.at[m], out_sem.at[m]).start()
        return []

    stages = (stage_stats, stage_dispatch, stage_up, stage_hidden, stage_down, stage_combine)
    crow[...] = jnp.zeros_like(crow)
    order = sorted(
        ((step + m, m, step) for m in range(micro) for step in range(len(stages)))
    )
    sent = []
    for _, m, step in order:
        copies = stages[step](m)
        if step not in (1, 4):
            for copy in copies:
                copy.start()
        sent += copies
    for copy in sent:
        copy.wait_send()
    for m in range(micro):
        to_sections(m, crow, in_crow, 0, "wait")
        to_sections(m, branch, in_branch, 1, "wait")
        pltpu.make_async_copy(obuf.at[m], out_ref.at[m], out_sem.at[m]).wait()


def body(paths_in, path_proj, coef_bias, norm_gain, w_gate_up, w_down, routes, route_gate):
    n_dp, n_ex, n_sec = (lax.axis_size(a) for a in ("dp", "expert", "section"))
    micro, rows, streams, width = paths_in.shape
    coefs, inner = path_proj.shape[1], w_down.shape[2]
    experts = n_ex // 2
    need = min(rows, max(2, -(-rows // experts)))
    cap = 16
    while cap < need:
        cap *= 2
    items, later = n_ex * cap, max(1, n_sec - 1)
    share = items // n_dp
    pairs = streams * (streams + 1) // 2
    stat_rows = -(-(coefs + pairs) // 8) * 8
    table = 2 * streams + 1 + streams * streams
    table_rows = -(-table // 8) * 8
    sizes = (micro, streams, rows, width, coefs, inner, cap, n_dp, n_ex, n_sec, width * n_dp)
    vmem, dma = pltpu.VMEM, pltpu.SemaphoreType.DMA
    scratch = [
        vmem((micro, streams, rows, width), BF16),
        vmem((width, 2 * inner), BF16),
        vmem((inner, width), BF16),
        vmem((micro, n_dp, stat_rows, rows), F32),
        vmem((micro, table_rows, LANES), F32),
        vmem((table, rows, LANES), F32),
        vmem((micro, rows, 1), F32),
        vmem((micro, experts, cap, width), BF16),
        vmem((micro, n_ex, cap, width), BF16),
        vmem((micro, n_dp, share, 2 * inner), F32),
        vmem((micro, n_dp, share, 2 * inner), BF16),
        vmem((micro, n_dp - 1, share, 2 * inner), BF16),
        vmem((micro, n_dp, share, inner), BF16),
        vmem((micro, n_ex, cap, width), BF16),
        vmem((micro, n_ex, cap, width), BF16),
        vmem((micro, rows, width), BF16),
        vmem((rows, width), F32),
        vmem((micro, later, table_rows, LANES), F32),
        vmem((micro, later, rows, width), BF16),
        vmem((micro, streams, rows, width), BF16),
        dma((micro + 2,)),
        dma((micro,)),
        *(dma((micro, n - 1)) for n in (n_dp, n_dp, n_ex, n_ex, n_dp, n_dp, n_dp, n_dp, n_ex, n_ex)),
        dma((micro, later, 2)),
        dma((micro, later, 2)),
    ]
    hbm, local = pl.BlockSpec(memory_space=pl.ANY), pl.BlockSpec(memory_space=pltpu.VMEM)
    out = pl.pallas_call(
        functools.partial(kernel, sizes),
        out_shape=jax.ShapeDtypeStruct((micro, streams, rows, width), BF16),
        in_specs=[hbm, local, local, local, hbm, hbm, local, local],
        out_specs=hbm,
        scratch_shapes=scratch,
        compiler_params=pltpu.CompilerParams(collective_id=0, has_side_effects=True),
    )(
        jnp.transpose(paths_in, (0, 2, 1, 3)),
        jnp.transpose(path_proj[0], (1, 0, 2)),
        coef_bias,
        norm_gain,
        w_gate_up[0, 0].reshape(width, -1),
        w_down[0, 0],
        routes[0],
        route_gate[0],
    )
    return jnp.transpose(out, (0, 2, 1, 3))[None]


def solution(mesh):
    in_specs = (
        P(None, "expert", None, "dp"),
        P("section", None, None, "dp"),
        P("section", None),
        P("section", "dp"),
        P("section", "expert", "dp", None, None),
        P("section", "expert", None, "dp"),
        P("section", None, "expert", None),
        P("section", None, "expert", None),
    )
    out_specs = P("section", None, "expert", None, "dp")
    return jax.shard_map(body, mesh=mesh, in_specs=in_specs, out_specs=out_specs, check_vma=False)
```

```python
import functools

import jax
import jax.numpy as jnp
from jax import lax
from jax.experimental import pallas as pl
from jax.experimental.pallas import tpu as pltpu
from jax.sharding import PartitionSpec as P

SINK = 20
EPSILON = 1e-06
MESH = pl.DeviceIdType.MESH
F32 = jnp.float32
BF16 = jnp.bfloat16
LANES = 128
NT = (((1,), (1,)), ((), ()))


def kernel(
    sizes,
    paths_ref, proj_ref, bias_ref, gain_ref, gate_up_ref, down_ref, routes_ref, gates_ref,
    out_ref,
    path, wgu, wd, stats, crow, tab, slotcol, outgoing, recv, acc, part, rs_recv, hid, half_out, ret,
    branch, acc_branch, in_crow, in_branch, obuf,
    load_sem, out_sem, st_s, st_r, di_s, di_r, rs_s, rs_r, ag_s, ag_r, re_s, re_r, se_s, se_r,
):
    micro, streams, rows, width, coefs, inner, cap, n_dp, n_ex, n_sec, depth = sizes
    experts = n_ex // 2
    slots = experts * cap
    items = n_ex * cap
    share = items // n_dp
    shift = cap.bit_length() - 1
    dp, ex, sec = (lax.axis_index(a) for a in ("dp", "expert", "section"))
    pre0, post0, scale0, mix0 = 0, streams, 2 * streams, 2 * streams + 1

    barrier = pltpu.get_barrier_semaphore()
    greeted = 0
    for name, me, count in (("dp", dp, n_dp), ("expert", ex, n_ex), ("section", sec, n_sec)):
        for off in range(1, count):
            pl.semaphore_signal(
                barrier, inc=1, device_id={name: lax.rem(me + off, count)}, device_id_type=MESH
            )
            greeted += 1

    loads = [
        pltpu.make_async_copy(paths_ref.at[m], path.at[m], load_sem.at[m]) for m in range(micro)
    ]
    load_gu = pltpu.make_async_copy(gate_up_ref, wgu, load_sem.at[micro])
    load_d = pltpu.make_async_copy(down_ref, wd, load_sem.at[micro + 1])
    for c in (*loads, load_gu, load_d):
        c.start()

    def remote(src, dst, send, receive, name, target):
        return pltpu.make_async_remote_copy(
            src_ref=src, dst_ref=dst, send_sem=send, recv_sem=receive,
            device_id={name: target}, device_id_type=MESH,
        )

    eye = lax.broadcasted_iota(jnp.int32, (rows, rows), 0) == lax.broadcasted_iota(
        jnp.int32, (rows, rows), 1
    )
    below = (
        lax.broadcasted_iota(jnp.int32, (rows, rows), 1)
        < lax.broadcasted_iota(jnp.int32, (rows, rows), 0)
    )

    def columns(table_ref, first, last):
        turned = jnp.transpose(table_ref[...])
        for k in range(first, last):
            tab[k] = jnp.broadcast_to(turned[:rows, k : k + 1], (rows, LANES))

    def mixed(m, c, added):
        cols = pl.ds(pl.multiple_of(c * LANES, LANES), LANES)
        p = [path[m, i, :, cols].astype(F32) for i in range(streams)]
        res = []
        for j in range(streams):
            total = tab[post0 + j] * added(cols)
            for i in range(streams):
                total = total + tab[mix0 + j * streams + i] * p[i]
            res.append(total.astype(BF16))
        return cols, res

    def stage_stats(m):
        loads[m].wait()
        for layer in range(n_sec - 1):
            @pl.when(sec > layer)
            def _():
                remote(crow.at[m], in_crow.at[m, layer], se_s.at[m, 0, 0],
                       se_r.at[m, layer, 0], "section", layer).wait_recv()
                columns(in_crow.at[m, layer], post0, mix0 + streams * streams)
                remote(branch.at[m], in_branch.at[m, layer], se_s.at[m, 0, 1],
                       se_r.at[m, layer, 1], "section", layer).wait_recv()

                @pl.loop(0, width // LANES, unroll=True)
                def _(c):
                    cols, res = mixed(m, c, lambda s: in_branch[m, layer, :, s].astype(F32))
                    for j in range(streams):
                        path[m, j, :, cols] = res[j]

        projected = jnp.zeros((coefs, rows), F32)
        at = coefs
        for j in range(streams):
            pj = path[m, j]
            projected = projected + lax.dot_general(
                proj_ref[j], pj, NT, preferred_element_type=F32
            )
            above = path[m, : j + 1].reshape((j + 1) * rows, width)
            g = lax.dot_general(above, pj, NT, preferred_element_type=F32)
            for i in range(j + 1):
                block = jnp.where(eye, g[i * rows : (i + 1) * rows], 0.0)
                stats[m, dp, at : at + 1, :] = jnp.sum(block, axis=0, keepdims=True)
                at += 1
        stats[m, dp, :coefs, :] = projected
        if m == 0:
            pl.semaphore_wait(barrier, greeted)
        return [
            remote(stats.at[m, dp], stats.at[m, dp], st_s.at[m, off - 1], st_r.at[m, off - 1],
                   "dp", lax.rem(dp + off, n_dp))
            for off in range(1, n_dp)
        ]

    def await_from(m, buf, sems, name, me, count):
        for off in range(1, count):
            source = lax.rem(me + count - off, count)
            remote(buf.at[m, source], buf.at[m, source], sems[0].at[m, off - 1],
                   sems[1].at[m, off - 1], name, source).wait_recv()

    def stage_dispatch(m):
        await_from(m, stats, (st_s, st_r), "dp", dp, n_dp)
        total = stats[m, 0]
        for d in range(1, n_dp):
            total = total + stats[m, d]
        gram, at = {}, coefs
        for j in range(streams):
            for i in range(j + 1):
                gram[i, j] = total[at : at + 1]
                at += 1
        square = gram[0, 0]
        for i in range(1, streams):
            square = square + gram[i, i]
        bias_eye = lax.broadcasted_iota(jnp.int32, (coefs, coefs), 0) == lax.broadcasted_iota(
            jnp.int32, (coefs, coefs), 1
        )
        bias = jnp.sum(jnp.where(bias_eye, bias_ref[...], 0.0), axis=1, keepdims=True)
        logits = total[:coefs] * lax.rsqrt(square * (1.0 / (streams * depth)) + EPSILON) + bias
        weights = jax.nn.sigmoid(logits[: 2 * streams])
        crow[m, pre0:streams, :rows] = weights[:streams]
        crow[m, post0 : 2 * streams, :rows] = 2.0 * weights[streams:]
        norm = jnp.zeros_like(square)
        for i, j in gram:
            pair = weights[i : i + 1] * weights[j : j + 1] * gram[i, j]
            norm = norm + (pair if i == j else 2.0 * pair)
        crow[m, scale0 : scale0 + 1, :rows] = lax.rsqrt(norm * (1.0 / depth) + EPSILON)
        columns(crow.at[m], pre0, scale0 + 1)

        route = routes_ref[m]
        lane = lax.broadcasted_iota(jnp.int32, (rows, LANES), 1)
        chosen = (lane == route).astype(F32)
        earlier = jnp.dot(
            below.astype(F32).astype(BF16), chosen.astype(BF16), preferred_element_type=F32
        )
        rank = jnp.sum(earlier * chosen, axis=1, keepdims=True)
        slot = route.astype(F32) * cap + rank
        slotcol[m] = slot
        slotrow = jnp.sum(jnp.where(eye, slot, 0.0), axis=0, keepdims=True)
        pick = (
            lax.broadcasted_iota(jnp.int32, (slots, rows), 0).astype(F32) == slotrow
        ).astype(F32).astype(BF16)

        @pl.loop(0, width // LANES, unroll=True)
        def _(c):
            cols = pl.ds(pl.multiple_of(c * LANES, LANES), LANES)
            merged = tab[pre0] * path[m, 0, :, cols].astype(F32)
            for i in range(1, streams):
                merged = merged + tab[pre0 + i] * path[m, i, :, cols].astype(F32)
            normed = (merged * tab[scale0] * gain_ref[:, cols].astype(F32)).astype(BF16)
            moved = jnp.dot(pick, normed, preferred_element_type=F32).astype(BF16)
            outgoing[m, :, :, cols] = moved.reshape(experts, cap, LANES)

        copies = []
        for off in range(1, n_ex):
            target = lax.rem(ex + off, n_ex)
            copies.append(
                remote(outgoing.at[m, lax.div(target, 2)], recv.at[m, ex], di_s.at[m, off - 1],
                       di_r.at[m, off - 1], "expert", target)
            )
            copies[-1].start()
        recv[m, ex] = outgoing[m, lax.div(ex, 2)]

        start = jnp.exp(logits[2 * streams :])
        entries = tuple(start[k : k + 1] for k in range(streams * streams))

        def balance(_, a):
            a = list(a)
            for groups in (
                [[j * streams + i for i in range(streams)] for j in range(streams)],
                [[j * streams + i for j in range(streams)] for i in range(streams)],
            ):
                for group in groups:
                    inverse = 1.0 / functools.reduce(jnp.add, [a[k] for k in group])
                    for k in group:
                        a[k] = a[k] * inverse
            return tuple(a)

        entries = lax.fori_loop(0, SINK, balance, entries)
        for k in range(streams * streams):
            crow[m, mix0 + k : mix0 + k + 1, :rows] = entries[k]
        to_sections(m, crow, in_crow, 0, "start")
        return copies

    def to_sections(m, src, dst, kind, act):
        for off in range(1, n_sec):
            @pl.when(sec + off < n_sec)
            def _():
                copy = remote(src.at[m], dst.at[m, sec], se_s.at[m, off - 1, kind],
                              se_r.at[m, sec, kind], "section", sec + off)
                copy.start() if act == "start" else copy.wait_send()

    def stage_up(m):
        await_from(m, recv, (di_s, di_r), "expert", ex, n_ex)
        if m == 0:
            load_gu.wait()
        tile = 256

        @pl.loop(0, 2 * inner // tile, unroll=True)
        def _(c):
            cols = pl.ds(pl.multiple_of(c * tile, tile), tile)
            product = jnp.dot(
                recv[m].reshape(items, width), wgu[:, cols], preferred_element_type=F32
            )
            acc[m, :, :, cols] = product.reshape(n_dp, share, tile)
            part[m, :, :, cols] = product.astype(BF16).reshape(n_dp, share, tile)

        return [
            remote(part.at[m, lax.rem(dp + off, n_dp)], rs_recv.at[m, off - 1],
                   rs_s.at[m, off - 1], rs_r.at[m, off - 1], "dp", lax.rem(dp + off, n_dp))
            for off in range(1, n_dp)
        ]

    def stage_hidden(m):
        for off in range(1, n_dp):
            remote(part.at[m, 0], rs_recv.at[m, off - 1], rs_s.at[m, off - 1],
                   rs_r.at[m, off - 1], "dp", lax.rem(dp + off, n_dp)).wait_recv()
        total = acc[m, dp]
        for off in range(1, n_dp):
            total = total + rs_recv[m, off - 1].astype(F32)
        gate = total[:, :inner]
        hid[m, dp] = (gate * jax.nn.sigmoid(gate) * total[:, inner:]).astype(BF16)
        return [
            remote(hid.at[m, dp], hid.at[m, dp], ag_s.at[m, off - 1], ag_r.at[m, off - 1],
                   "dp", lax.rem(dp + off, n_dp))
            for off in range(1, n_dp)
        ]

    def stage_down(m):
        await_from(m, hid, (ag_s, ag_r), "dp", dp, n_dp)
        if m == 0:
            load_d.wait()
        tile = 256 if width % 256 == 0 else LANES

        @pl.loop(0, width // tile, unroll=True)
        def _(c):
            cols = pl.ds(pl.multiple_of(c * tile, tile), tile)
            product = jnp.dot(
                hid[m].reshape(items, inner), wd[:, cols], preferred_element_type=F32
            )
            half_out[m, :, :, cols] = product.astype(BF16).reshape(n_ex, cap, tile)

        copies = [
            remote(half_out.at[m, lax.rem(ex + off, n_ex)], ret.at[m, ex], re_s.at[m, off - 1],
                   re_r.at[m, off - 1], "expert", lax.rem(ex + off, n_ex))
            for off in range(1, n_ex)
        ]
        for copy in copies:
            copy.start()
        ret[m, ex] = half_out[m, ex]
        return copies

    def stage_combine(m):
        columns(crow.at[m], post0, mix0 + streams * streams)
        place = lax.broadcasted_iota(jnp.int32, (rows, items), 1)
        place = ((place >> (shift + 1)) << shift) + (place & (cap - 1))
        back = (place.astype(F32) == slotcol[m]).astype(F32).astype(BF16)
        gates = gates_ref[m]
        await_from(m, ret, (re_s, re_r), "expert", ex, n_ex)
        tile = 256 if width % 256 == 0 else LANES

        @pl.loop(0, width // tile, unroll=True)
        def _(c):
            cols = pl.ds(pl.multiple_of(c * tile, tile), tile)
            value = gates * jnp.dot(
                back, ret[m, :, :, cols].reshape(items, tile), preferred_element_type=F32
            )
            acc_branch[:, cols] = value
            branch[m, :, cols] = value.astype(BF16)

        to_sections(m, branch, in_branch, 1, "start")

        @pl.loop(0, width // LANES, unroll=True)
        def _(c):
            cols, res = mixed(m, c, lambda s: acc_branch[:, s])
            for j in range(streams):
                obuf[m, j, :, cols] = res[j]

        pltpu.make_async_copy(obuf.at[m], out_ref.at[m], out_sem.at[m]).start()
        return []

    stages = (stage_stats, stage_dispatch, stage_up, stage_hidden, stage_down, stage_combine)
    crow[...] = jnp.zeros_like(crow)
    order = sorted(
        ((step + m, m, step) for m in range(micro) for step in range(len(stages)))
    )
    sent = []
    for _, m, step in order:
        copies = stages[step](m)
        if step not in (1, 4):
            for copy in copies:
                copy.start()
        sent += copies
    for copy in sent:
        copy.wait_send()
    for m in range(micro):
        to_sections(m, crow, in_crow, 0, "wait")
        to_sections(m, branch, in_branch, 1, "wait")
        pltpu.make_async_copy(obuf.at[m], out_ref.at[m], out_sem.at[m]).wait()


def body(paths_in, path_proj, coef_bias, norm_gain, w_gate_up, w_down, routes, route_gate):
    n_dp, n_ex, n_sec = (lax.axis_size(a) for a in ("dp", "expert", "section"))
    micro, rows, streams, width = paths_in.shape
    coefs, inner = path_proj.shape[1], w_down.shape[2]
    experts = n_ex // 2
    need = min(rows, max(2, -(-rows // experts)))
    cap = 16
    while cap < need:
        cap *= 2
    items, later = n_ex * cap, max(1, n_sec - 1)
    share = items // n_dp
    pairs = streams * (streams + 1) // 2
    stat_rows = -(-(coefs + pairs) // 8) * 8
    table = 2 * streams + 1 + streams * streams
    table_rows = -(-table // 8) * 8
    sizes = (micro, streams, rows, width, coefs, inner, cap, n_dp, n_ex, n_sec, width * n_dp)
    vmem, dma = pltpu.VMEM, pltpu.SemaphoreType.DMA
    scratch = [
        vmem((micro, streams, rows, width), BF16),
        vmem((width, 2 * inner), BF16),
        vmem((inner, width), BF16),
        vmem((micro, n_dp, stat_rows, rows), F32),
        vmem((micro, table_rows, LANES), F32),
        vmem((table, rows, LANES), F32),
        vmem((micro, rows, 1), F32),
        vmem((micro, experts, cap, width), BF16),
        vmem((micro, n_ex, cap, width), BF16),
        vmem((micro, n_dp, share, 2 * inner), F32),
        vmem((micro, n_dp, share, 2 * inner), BF16),
        vmem((micro, n_dp - 1, share, 2 * inner), BF16),
        vmem((micro, n_dp, share, inner), BF16),
        vmem((micro, n_ex, cap, width), BF16),
        vmem((micro, n_ex, cap, width), BF16),
        vmem((micro, rows, width), BF16),
        vmem((rows, width), F32),
        vmem((micro, later, table_rows, LANES), F32),
        vmem((micro, later, rows, width), BF16),
        vmem((micro, streams, rows, width), BF16),
        dma((micro + 2,)),
        dma((micro,)),
        *(dma((micro, n - 1)) for n in (n_dp, n_dp, n_ex, n_ex, n_dp, n_dp, n_dp, n_dp, n_ex, n_ex)),
        dma((micro, later, 2)),
        dma((micro, later, 2)),
    ]
    hbm, local = pl.BlockSpec(memory_space=pl.ANY), pl.BlockSpec(memory_space=pltpu.VMEM)
    out = pl.pallas_call(
        functools.partial(kernel, sizes),
        out_shape=jax.ShapeDtypeStruct((micro, streams, rows, width), BF16),
        in_specs=[hbm, local, local, local, hbm, hbm, local, local],
        out_specs=hbm,
        scratch_shapes=scratch,
        compiler_params=pltpu.CompilerParams(collective_id=0, has_side_effects=True),
    )(
        jnp.transpose(paths_in, (0, 2, 1, 3)),
        jnp.transpose(path_proj[0], (1, 0, 2)),
        coef_bias,
        norm_gain,
        w_gate_up[0, 0].reshape(width, -1),
        w_down[0, 0],
        routes[0],
        route_gate[0],
    )
    return jnp.transpose(out, (0, 2, 1, 3))[None]


def solution(mesh):
    in_specs = (
        P(None, "expert", None, "dp"),
        P("section", None, None, "dp"),
        P("section", None),
        P("section", "dp"),
        P("section", "expert", "dp", None, None),
        P("section", "expert", None, "dp"),
        P("section", None, "expert", None),
        P("section", None, "expert", None),
    )
    out_specs = P("section", None, "expert", None, "dp")
    return jax.shard_map(body, mesh=mesh, in_specs=in_specs, out_specs=out_specs, check_vma=False)
```
